512 devices in a mesh: task: 4 (over y_lo), tok: 128 (over z, y_hi, x, core).
Axes of the slice: x: 4, y: 8 (y_hi: 2, y_lo: 4; y = y_hi * 4 + y_lo), z: 8, core: 2. Of those that a mesh axis runs over, the one named last changes fastest.
Arguments:
- hidden: bfloat16 [4, 4096, 3584], P('task', 'tok'), may hold values from -6 to 6
- attn_out: bfloat16 [4, 4096, 3584], P('task', 'tok'), may hold values from -6 to 6
- gain_attn: bfloat16 [3584], replicated, may hold values from 0.5 to 1.5
- gain_mlp: bfloat16 [3584], replicated, may hold values from 0.5 to 1.5
- lengths: int32 [4, 2], P('task'), may hold values from 512 to 2048
Outputs:
- gram_attn: float32 [128, 112, 896], P('tok', 'task')
- gram_mlp: float32 [128, 112, 896], P('tok', 'task')
The draws below stay inside these ranges and needn't reach their ends.
All inputs are finite; a program needn't handle non-finite values.
Results may differ from the reference program's by a relative error of at most 0.0044.
Values may be sent and summed in bfloat16 or wider, within the bound.
No kernel may reach another device: no remote copies, remote signals or barrier semaphores. Data moves between devices by JAX's collectives and lax.ppermute only.
A program may use at most 64 MiB of HBM per device.

```python
import jax
import jax.numpy as jnp
from jax import lax

D = 3584
SEQS = 2
BSIDE = 4
BW = 896
PR = 112
TOKENS = 4096
SEQ_LEN = 2048
N_TASK = 4
N_TOK = 128


def with_ends(result, stream_key, smallest, largest):
    longest = result.shape.index(max(result.shape))
    spots = []
    for shift in (0, 1):
        where = [jax.random.randint(jax.random.fold_in(stream_key, axis), (), 0, length) for axis, length in enumerate(result.shape)]
        where[longest] = (where[longest] + shift) % result.shape[longest]
        spots.append(tuple(where))
    return result.at[spots[0]].set(smallest).at[spots[1]].set(largest)


def block_levels(stream_key, shape, shards, least, high):
    loudness = 1.0
    for position, blocks in shards:
        steps = jax.random.uniform(jax.random.fold_in(jax.random.fold_in(stream_key, 6), position), (blocks,), jnp.float32, least / len(shards), high / len(shards))
        loudness = loudness * jnp.repeat(jnp.exp(steps), shape[position] // blocks).reshape((-1,) + (1,) * (len(shape) - 1 - position))
    return loudness


def scatter_about(rng, dims, scale, most, split=(), kind=jnp.bfloat16):
    drawn = scale * jax.random.normal(rng, dims, jnp.float32)
    if split:
        drawn = drawn * block_levels(rng, dims, split, -0.22, 0.18)
    return jnp.clip(drawn, -most, most).astype(kind)


def setup_inputs(seed: int = 0) -> dict:
    key_list = jax.random.split(jax.random.key(seed), 6)
    return {
        "hidden": scatter_about(key_list[0], (N_TASK, TOKENS, D), 1.0, 6.0, ((0, 4), (1, 128))),
        "attn_out": scatter_about(key_list[1], (N_TASK, TOKENS, D), 1.0, 6.0, ((0, 4), (1, 128))),
        "gain_attn": jnp.clip(1.0 + 0.1 * jax.random.normal(key_list[2], (D,), jnp.float32), 0.5, 1.5).astype(jnp.bfloat16),
        "gain_mlp": jnp.clip(1.0 + 0.1 * jax.random.normal(key_list[3], (D,), jnp.float32), 0.5, 1.5).astype(jnp.bfloat16),
        "lengths": with_ends(jax.random.randint(key_list[4], (N_TASK, SEQS), SEQ_LEN // 4, SEQ_LEN + 1), jax.random.fold_in(key_list[4], 1), SEQ_LEN // 4, SEQ_LEN).astype(jnp.int32),
    }


def normed(values, gain):
    scale = lax.rsqrt(lax.optimization_barrier(jnp.mean(values * values, axis=-1, keepdims=True)) + 1e-06)
    return values * scale * gain.astype(jnp.float32)

def reference(hidden, attn_out, gain_attn, gain_mlp, lengths):
    place = jnp.arange(TOKENS, dtype=jnp.int32)
    which = place // SEQ_LEN
    offset = place % SEQ_LEN
    total_attn = jnp.zeros((D, D), jnp.float32)
    total_mlp = jnp.zeros((D, D), jnp.float32)
    for group in range(N_TASK):
        limit = lengths[group][which]
        live = (offset < limit).astype(jnp.float32)[:, None]
        first = hidden[group].astype(jnp.float32)
        x_attn = (normed(first, gain_attn) * live).astype(jnp.bfloat16)
        mixed = first + attn_out[group].astype(jnp.float32)
        x_mlp = (normed(mixed, gain_mlp) * live).astype(jnp.bfloat16)
        total_attn = total_attn + jnp.dot(x_attn.T, x_attn, preferred_element_type=jnp.float32)
        total_mlp = total_mlp + jnp.dot(x_mlp.T, x_mlp, preferred_element_type=jnp.float32)

    def tiled(total):
        gram = total / TOKENS
        blocks = gram.reshape(BSIDE, BW, BSIDE, BW).transpose(0, 2, 1, 3)
        return blocks.reshape(N_TOK, PR, BW)
    return (tiled(total_attn), tiled(total_mlp))
```

```python
import jax
import jax.numpy as jnp
from jax import lax
from jax.sharding import Mesh
from jax.sharding import PartitionSpec as P

TOK = ("z", "yh", "x", "core")
YRING = ("yh", "task")


def normed(values, gain):
    scale = lax.rsqrt(jnp.mean(values * values, axis=-1, keepdims=True) + 1e-06)
    return values * scale * gain.astype(jnp.float32)


def per_device(hidden, attn_out, gain_attn, gain_mlp, lengths):
    rows = hidden.shape[1]
    width = hidden.shape[2]
    n_z, n_yh, n_x, n_core = (lax.axis_size(a) for a in TOK)
    n_task = lax.axis_size("task")
    tokens = rows * n_z * n_yh * n_x * n_core
    seq_len = tokens // lengths.shape[1]
    band = width // 4
    part = band // (n_x * n_core * n_task)
    z = lax.axis_index("z")
    core = lax.axis_index("core")

    place = lax.axis_index(TOK) * rows + jnp.arange(rows, dtype=jnp.int32)
    which = lax.axis_index(TOK) * rows // seq_len
    limit = lax.dynamic_index_in_dim(lengths[0], which, keepdims=False)
    live = (place - which * seq_len < limit).astype(jnp.float32)[:, None]
    first = hidden[0].astype(jnp.float32)
    x_attn = (normed(first, gain_attn) * live).astype(jnp.bfloat16)
    mixed = first + attn_out[0].astype(jnp.float32)
    x_mlp = (normed(mixed, gain_mlp) * live).astype(jnp.bfloat16)

    both = jnp.concatenate([x_attn, x_mlp], axis=1)
    seen = lax.all_gather(both, ("z", "core"), axis=0, tiled=True)

    def tile(at):
        left = lax.dynamic_slice_in_dim(seen, at * width + z // 2 * band, band, 1)
        right = lax.dynamic_slice_in_dim(seen, at * width + z % 2 * 2 * band, 2 * band, 1)
        full = lax.dot_general(
            left, right, (((0,), (0,)), ((), ())), preferred_element_type=jnp.float32
        )
        full = full.reshape(n_x, n_core, n_task, part, n_yh, band)
        return jnp.where(core == 0, full[:, 0], full[:, 1])

    parts = jnp.stack([tile(0), tile(1)])
    parts = parts.transpose(4, 2, 1, 0, 3, 5).astype(jnp.bfloat16)
    parts = parts.reshape(n_yh * n_task * n_x * 2 * part, band)
    ring = lax.psum_scatter(parts, YRING, scatter_dimension=0, tiled=True)
    ring = ring.reshape(n_x, 2 * part, band)
    ring = lax.all_to_all(ring, "x", split_axis=0, concat_axis=0, tiled=True)
    total = ring.astype(jnp.float32).sum(axis=0) * (1.0 / tokens)
    return total[None, :part], total[None, part:]


def solution(mesh):
    n_task = mesh.shape["task"]
    grid = Mesh(mesh.devices.reshape(n_task, 8, 2, 4, 2), ("task",) + TOK)
    return jax.shard_map(
        per_device,
        mesh=grid,
        in_specs=(P("task", TOK, None), P("task", TOK, None), P(), P(), P("task", None)),
        out_specs=(P(TOK, "task", None), P(TOK, "task", None)),
        check_vma=False,
    )
```

```python
import jax
import jax.numpy as jnp
import numpy as np
from jax import lax
from jax.sharding import Mesh
from jax.sharding import PartitionSpec as P

TOK = ("z", "yh", "x", "core")
ALL = ("task",) + TOK
YRING = ("yh", "task")
PAIRS = ((0, 1), (0, 2), (0, 3), (1, 2), (1, 3), (2, 3), (0, 1), (2, 3))
MIXED = 6


def tile_of(pair, core):
    i, j = PAIRS[pair]
    if pair < MIXED:
        return (i, j) if core == 0 else (j, i)
    return (i, i) if core == 0 else (j, j)


def home_routes(shape):
    flat = np.arange(np.prod(shape)).reshape(shape)
    by_z, by_y = [], []
    for t, z, yh, x, core in np.ndindex(*shape):
        here = int(flat[t, z, yh, x, core])
        i, j = tile_of(z, core)
        by_z.append((here, int(flat[t, 2 * i + j // 2, j % 2, x, yh])))
        i, j = tile_of(yh * shape[0] + t, core)
        by_y.append((here, int(flat[z % 4, 2 * i + j // 2, j % 2, x, z // 4])))
    return by_z, by_y


def normed(values, gain):
    scale = lax.rsqrt(jnp.mean(values * values, axis=-1, keepdims=True) + 1e-06)
    return values * scale * gain.astype(jnp.float32)


def solution(mesh):
    shape = (mesh.shape["task"], 8, 2, 4, 2)
    grid = Mesh(mesh.devices.reshape(shape), ALL)
    by_z, by_y = home_routes(shape)

    def per_device(hidden, attn_out, gain_attn, gain_mlp, lengths):
        rows = hidden.shape[1]
        width = hidden.shape[2]
        n_x = lax.axis_size("x")
        tokens = rows * lax.axis_size(TOK)
        seq_len = tokens // lengths.shape[1]
        band = width // 4
        core = lax.axis_index("core")

        start = lax.axis_index(TOK) * rows
        which = start // seq_len
        limit = lax.dynamic_index_in_dim(lengths[0], which, keepdims=False)
        place = start - which * seq_len + jnp.arange(rows, dtype=jnp.int32)
        live = (place < limit).astype(jnp.float32)[:, None]
        first = hidden[0].astype(jnp.float32)
        x_attn = (normed(first, gain_attn) * live).astype(jnp.bfloat16)
        mixed = first + attn_out[0].astype(jnp.float32)
        x_mlp = (normed(mixed, gain_mlp) * live).astype(jnp.bfloat16)

        def spread(values, ring):
            cut = [values[:, b * band : (b + 1) * band] for b in range(4)]
            out = jnp.stack([jnp.concatenate([cut[i], cut[j]], axis=1) for i, j in PAIRS])
            return lax.all_to_all(out, ring, split_axis=0, concat_axis=0, tiled=True)

        def tile(own, pair):
            own = own.reshape(-1, 2 * band)
            other = lax.ppermute(own, "core", [(0, 1), (1, 0)])
            side = jnp.where((core == 0) == (pair < MIXED), 1, 0)

            def product(seen):
                left = lax.dynamic_slice_in_dim(seen, core * band, band, 1)
                right = lax.dynamic_slice_in_dim(seen, side * band, band, 1)
                return lax.dot_general(
                    left, right, (((0,), (0,)), ((), ())), preferred_element_type=jnp.float32
                )

            return (product(own) + product(other)).astype(jnp.bfloat16)

        def reduced(part, ring, count):
            part = part.reshape(count, -1, band)
            got = lax.all_to_all(part, ring, split_axis=0, concat_axis=0, tiled=True)
            return got.astype(jnp.float32).sum(axis=0)

        got_attn = spread(x_attn, "z")
        got_mlp = spread(x_mlp, YRING)
        part_attn = tile(got_attn, lax.axis_index("z"))
        part_mlp = tile(got_mlp, lax.axis_index(YRING))
        half_attn = reduced(part_attn, "x", n_x).astype(jnp.bfloat16)
        half_mlp = reduced(part_mlp, "x", n_x).astype(jnp.bfloat16)
        scale = 1.0 / tokens
        end_attn = (reduced(half_attn, YRING, 8) * scale).astype(jnp.bfloat16)
        end_mlp = (reduced(half_mlp, "z", 8) * scale).astype(jnp.bfloat16)
        home_attn = lax.ppermute(end_attn, ALL, by_z)
        home_mlp = lax.ppermute(end_mlp, ALL, by_y)
        return home_attn.astype(jnp.float32)[None], home_mlp.astype(jnp.float32)[None]

    return jax.shard_map(
        per_device,
        mesh=grid,
        in_specs=(P("task", TOK, None), P("task", TOK, None), P(), P(), P("task", None)),
        out_specs=(P(TOK, "task", None), P(TOK, "task", None)),
        check_vma=False,
    )
```

```python
import jax
import jax.numpy as jnp
import numpy as np
from jax import lax
from jax.experimental import pallas as pl
from jax.experimental.pallas import tpu as pltpu
from jax.sharding import Mesh
from jax.sharding import PartitionSpec as P

TOK = ("z", "yh", "x", "core")
ALL = ("task",) + TOK
YRING = ("yh", "task")
PAIRS = ((0, 1), (0, 2), (0, 3), (1, 2), (1, 3), (2, 3), (0, 1), (2, 3))
MIXED = 6
FAR = (4, 3, 5, 2, 6, 1, 7)


def tile_of(pair, core):
    i, j = PAIRS[pair]
    if pair < MIXED:
        return (i, j) if core == 0 else (j, i)
    return (i, i) if core == 0 else (j, j)


def home_routes(shape):
    flat = np.arange(np.prod(shape)).reshape(shape)
    by_z, by_y = [], []
    for t, z, yh, x, core in np.ndindex(*shape):
        here = int(flat[t, z, yh, x, core])
        i, j = tile_of(z, core)
        by_z.append((here, int(flat[t, 2 * i + j // 2, j % 2, x, yh])))
        i, j = tile_of(yh * shape[0] + t, core)
        by_y.append((here, int(flat[x, 2 * i + j // 2, j % 2, z // 2, z % 2])))
    return by_z, by_y


def normed(values, gain, live):
    scale = lax.rsqrt(jnp.mean(values * values, axis=-1, keepdims=True) + 1e-06)
    return (values * scale * gain * live).astype(jnp.bfloat16)


def norm_kernel(live_ref, hidden_ref, extra_ref, gain_ref, attn_ref, *rest):
    mlp_refs, mlp_x = rest[:-1], rest[-1]
    rows = hidden_ref.shape[0]
    band = hidden_ref.shape[1] // 4
    live = (lax.broadcasted_iota(jnp.int32, (rows, 1), 0) < live_ref[0]).astype(jnp.float32)
    first = hidden_ref[...].astype(jnp.float32)
    x_attn = normed(first, gain_ref[0:1, :], live)
    for p, (i, j) in enumerate(PAIRS):
        attn_ref[p, :, :band] = x_attn[:, i * band : (i + 1) * band]
        attn_ref[p, :, band:] = x_attn[:, j * band : (j + 1) * band]
    mixed = first + extra_ref[...].astype(jnp.float32)
    mlp_x[...] = normed(mixed, gain_ref[1:2, :], live)
    for d, ref in enumerate(mlp_refs):
        q = (live_ref[1] + d) % len(PAIRS)
        i = jnp.where(q < 3, 0, jnp.where(q < 5, 1, jnp.where(q == 6, 0, 2)))
        j = jnp.where((q == 0) | (q == 6), 1, jnp.where((q == 1) | (q == 3), 2, 3))
        ref[:, :band] = mlp_x[:, pl.ds(pl.multiple_of(i * band, 128), band)]
        ref[:, band:] = mlp_x[:, pl.ds(pl.multiple_of(j * band, 128), band)]


def norms(facts, hidden, extra, gains):
    rows, width = hidden.shape
    block = jax.ShapeDtypeStruct((rows, width // 2), jnp.bfloat16)
    vmem = pl.BlockSpec(memory_space=pltpu.VMEM)
    return pl.pallas_call(
        norm_kernel,
        out_shape=(jax.ShapeDtypeStruct((8, rows, width // 2), jnp.bfloat16),) + (block,) * 8,
        in_specs=[pl.BlockSpec(memory_space=pltpu.SMEM), vmem, vmem, vmem],
        out_specs=(vmem,) * 9,
        scratch_shapes=[pltpu.VMEM((rows, width), jnp.bfloat16)],
    )(facts, hidden, extra, gains)


def solution(mesh):
    shape = (mesh.shape["task"], 8, 2, 4, 2)
    grid = Mesh(mesh.devices.reshape(shape), ALL)
    by_z, by_y = home_routes(shape)
    n_task = shape[0]
    y_routes = [
        [(s % n_task * 2 + s // n_task, r % n_task * 2 + r // n_task) for s, r in pairs]
        for pairs in ([(s, (s + d) % 8) for s in range(8)] for d in range(8))
    ]

    def per_device(hidden, attn_out, gain_attn, gain_mlp, lengths):
        rows = hidden.shape[1]
        width = hidden.shape[2]
        n_x = lax.axis_size("x")
        tokens = rows * lax.axis_size(TOK)
        seq_len = tokens // lengths.shape[1]
        band = width // 4
        core = lax.axis_index("core")

        start = lax.axis_index(TOK) * rows
        which = start // seq_len
        limit = lax.dynamic_index_in_dim(lengths[0], which, keepdims=False)
        y = lax.axis_index(YRING)
        facts = jnp.stack([limit - (start - which * seq_len), y])
        gains = jnp.stack([gain_attn, gain_mlp]).astype(jnp.float32)
        to_attn, *to_mlp = norms(facts, hidden[0], attn_out[0], gains)

        def tile(own, pair):
            own = own.reshape(-1, 2 * band)
            other = lax.ppermute(own, "core", [(0, 1), (1, 0)])
            side = jnp.where((core == 0) == (pair < MIXED), 1, 0)

            def product(seen):
                left = lax.dynamic_slice_in_dim(seen, core * band, band, 1)
                right = lax.dynamic_slice_in_dim(seen, side * band, band, 1)
                return lax.dot_general(
                    left, right, (((0,), (0,)), ((), ())), preferred_element_type=jnp.float32
                )

            return (product(own) + product(other)).astype(jnp.bfloat16)

        def swapped(part, ring, count):
            part = part.reshape(count, -1, part.shape[-1])
            return lax.all_to_all(part, ring, split_axis=0, concat_axis=0, tiled=True)

        def summed(got):
            return got.astype(jnp.float32).sum(axis=0)

        def sent(part, axis, at, count, order):
            part = part.reshape(count, -1, band)
            total = lax.dynamic_index_in_dim(part, at, 0, False).astype(jnp.float32)
            for d in order:
                piece = lax.dynamic_index_in_dim(part, (at + d) % count, 0, False)
                piece = lax.ppermute(piece, axis, [(s, (s + d) % count) for s in range(count)])
                total = total + piece.astype(jnp.float32)
            return total

        got_attn = swapped(to_attn, "z", 8)
        got_mlp = [to_mlp[0]]
        for d in FAR:
            got_mlp.append(lax.ppermute(to_mlp[d], ("task", "yh"), y_routes[d]))
        part_attn = tile(got_attn, lax.axis_index("z"))
        part_mlp = tile(jnp.concatenate(got_mlp), y)
        half_attn = summed(swapped(part_attn, "x", n_x)).astype(jnp.bfloat16)
        half_mlp = sent(part_mlp, "z", lax.axis_index("z"), 8, FAR).astype(jnp.bfloat16)
        scale = 1.0 / tokens
        end_attn = (summed(swapped(half_attn, YRING, 8)) * scale).astype(jnp.bfloat16)
        end_mlp = sent(half_mlp, "x", lax.axis_index("x"), n_x, (2, 1, 3)) * scale
        home_attn = lax.ppermute(end_attn, ALL, by_z)
        home_mlp = lax.ppermute(end_mlp.astype(jnp.bfloat16), ALL, by_y)
        return home_attn.astype(jnp.float32)[None], home_mlp.astype(jnp.float32)[None]

    return jax.shard_map(
        per_device,
        mesh=grid,
        in_specs=(P("task", TOK, None), P("task", TOK, None), P(), P(), P("task", None)),
        out_specs=(P(TOK, "task", None), P(TOK, "task", None)),
        check_vma=False,
    )
```

```python
import jax
import jax.numpy as jnp
import numpy as np
from jax import lax
from jax.experimental import pallas as pl
from jax.experimental.pallas import tpu as pltpu
from jax.sharding import Mesh
from jax.sharding import PartitionSpec as P

TOK = ("z", "yh", "x", "core")
ALL = ("task",) + TOK
YRING = ("yh", "task")
PAIRS = ((0, 1), (0, 2), (0, 3), (1, 2), (1, 3), (2, 3), (0, 1), (2, 3))
MIXED = 6
VMEM = pl.BlockSpec(memory_space=pltpu.VMEM)
SMEM = pl.BlockSpec(memory_space=pltpu.SMEM)


def tile_of(pair, second):
    i, j = PAIRS[pair]
    if pair < MIXED:
        return (j, i) if second else (i, j)
    return (j, j) if second else (i, i)


def routes(shape):
    n_task, n_z, n_yh, n_x, n_core = shape
    flat = np.arange(np.prod(shape)).reshape(shape)
    z_first, y_first = [], []
    for t, yh, x in np.ndindex(n_task, n_yh, n_x):
        z_first.append([int(d) for d in flat[t, :, yh, x, 0]])
        y_first.append([int(d) for d in flat[t, :, yh, x, 1]])
    for z, x in np.ndindex(n_z, n_x):
        for core, groups in ((1, z_first), (0, y_first)):
            groups.append([int(d) for yh in range(n_yh) for d in flat[:, z, yh, x, core]])
    homes = ([], [])
    for t, z, yh, x, core in np.ndindex(*shape):
        y = yh * n_task + t
        pair, rows = (z, y) if core == 0 else (y, z)
        for n in range(2):
            i, j = tile_of(pair, n != core)
            home = flat[x, 2 * i + j // 2, j % 2, rows // n_core, rows % n_core]
            homes[n].append((int(flat[t, z, yh, x, core]), int(home)))
    return z_first, y_first, homes


def normed(values, gain, live):
    scale = lax.rsqrt(jnp.mean(values * values, axis=-1, keepdims=True) + 1e-06)
    return (values * scale * gain * live).astype(jnp.bfloat16)


def norm_kernel(facts_ref, hidden_ref, extra_ref, gain_ref, keep_ref, send_ref):
    rows = hidden_ref.shape[0]
    live = (lax.broadcasted_iota(jnp.int32, (rows, 1), 0) < facts_ref[0]).astype(jnp.float32)
    first = hidden_ref[...].astype(jnp.float32)
    x_attn = normed(first, gain_ref[0:1, :], live)
    mixed = first + extra_ref[...].astype(jnp.float32)
    x_mlp = normed(mixed, gain_ref[1:2, :], live)

    @pl.when(facts_ref[1] == 0)
    def _():
        keep_ref[...] = x_attn
        send_ref[...] = x_mlp

    @pl.when(facts_ref[1] != 0)
    def _():
        keep_ref[...] = x_mlp
        send_ref[...] = x_attn


def norms(facts, hidden, extra, gains):
    block = jax.ShapeDtypeStruct(hidden.shape, jnp.bfloat16)
    return pl.pallas_call(
        norm_kernel,
        out_shape=(block, block),
        in_specs=[SMEM, VMEM, VMEM, VMEM],
        out_specs=(VMEM, VMEM),
    )(facts, hidden, extra, gains)


def deal_kernel(keep_ref, got_ref, out_ref):
    rows = keep_ref.shape[0]
    band = keep_ref.shape[1] // 4
    for p, pair in enumerate(PAIRS):
        for n, b in enumerate(pair):
            lanes = slice(n * band, (n + 1) * band)
            out_ref[p, :rows, lanes] = keep_ref[:, b * band : (b + 1) * band]
            out_ref[p, rows:, lanes] = got_ref[:, b * band : (b + 1) * band]


def dealt(keep, got):
    rows, width = keep.shape
    return pl.pallas_call(
        deal_kernel,
        out_shape=jax.ShapeDtypeStruct((len(PAIRS), 2 * rows, width // 2), jnp.bfloat16),
        in_specs=[VMEM, VMEM],
        out_specs=VMEM,
    )(keep, got)


def gram_kernel(facts_ref, seen_ref, out_ref):
    band = seen_ref.shape[1] // 2
    rows = band // len(PAIRS)
    for n in range(2):
        at = facts_ref[2] if n == 0 else 1 - facts_ref[2]
        right = seen_ref[:, pl.ds(pl.multiple_of(at * band, 128), band)]
        full = lax.dot_general(
            seen_ref[:, n * band : (n + 1) * band],
            right,
            (((0,), (0,)), ((), ())),
            preferred_element_type=jnp.float32,
        )
        for k in range(len(PAIRS)):
            part = full[k * rows : (k + 1) * rows].astype(jnp.bfloat16)
            out_ref[k, n * rows : (n + 1) * rows, :] = part


def grams(facts, seen):
    band = seen.shape[1] // 2
    return pl.pallas_call(
        gram_kernel,
        out_shape=jax.ShapeDtypeStruct((len(PAIRS), 2 * band // len(PAIRS), band), jnp.bfloat16),
        in_specs=[SMEM, VMEM],
        out_specs=VMEM,
    )(facts, seen)


def solution(mesh):
    shape = (mesh.shape["task"], 8, 2, 4, 2)
    grid = Mesh(mesh.devices.reshape(shape), ALL)
    z_first, y_first, homes = routes(shape)

    def per_device(hidden, attn_out, gain_attn, gain_mlp, lengths):
        rows = hidden.shape[1]
        band = hidden.shape[2] // 4
        n_x = lax.axis_size("x")
        tokens = rows * lax.axis_size(TOK)
        seq_len = tokens // lengths.shape[1]
        core = lax.axis_index("core")
        z = lax.axis_index("z")
        yh = lax.axis_index("yh")

        start = lax.axis_index(TOK) * rows
        which = start // seq_len
        limit = lax.dynamic_index_in_dim(lengths[0], which, keepdims=False)
        pair = jnp.where(core == 0, z, lax.axis_index(YRING))
        facts = jnp.stack(
            [limit - (start - which * seq_len), core, (pair < MIXED).astype(jnp.int32)]
        )
        gains = jnp.stack([gain_attn, gain_mlp]).astype(jnp.float32)

        def swapped(part, groups):
            return lax.all_to_all(
                part, ALL, split_axis=0, concat_axis=0, axis_index_groups=groups, tiled=True
            )

        keep, send = norms(facts, hidden[0], attn_out[0], gains)
        got = lax.ppermute(send, "core", [(0, 1), (1, 0)])
        seen = swapped(dealt(keep, got), z_first).reshape(-1, 2 * band)
        part = swapped(grams(facts, seen), y_first)
        half = part.astype(jnp.float32).sum(axis=0).reshape(2, n_x, -1, band)
        half = half.transpose(1, 0, 2, 3).reshape(n_x, -1, band).astype(jnp.bfloat16)
        last = lax.all_to_all(half, "x", split_axis=0, concat_axis=0, tiled=True)
        last = last.astype(jnp.float32).sum(axis=0).reshape(2, -1, band) * (1.0 / tokens)
        last = last.astype(jnp.bfloat16)
        same = lax.ppermute(jnp.where(core == 0, last[0], last[1]), ALL, homes[0])
        other = lax.ppermute(jnp.where(core == 0, last[1], last[0]), ALL, homes[1])
        i, j = z // 2, z % 2 * 2 + yh
        upper = (i < j) | ((i == j) & (i % 2 == 0))
        out_attn = jnp.where(upper, same, other).astype(jnp.float32)
        out_mlp = jnp.where(upper, other, same).astype(jnp.float32)
        return out_attn[None], out_mlp[None]

    return jax.shard_map(
        per_device,
        mesh=grid,
        in_specs=(P("task", TOK, None), P("task", TOK, None), P(), P(), P("task", None)),
        out_specs=(P(TOK, "task", None), P(TOK, "task", None)),
        check_vma=False,
    )
```

```python
import jax
import jax.numpy as jnp
import numpy as np
from jax import lax
from jax.experimental import pallas as pl
from jax.experimental.pallas import tpu as pltpu
from jax.sharding import Mesh
from jax.sharding import PartitionSpec as P

TOK = ("z", "yh", "x", "core")
ALL = ("task",) + TOK
YRING = ("yh", "task")
PAIRS = ((0, 1), (0, 2), (0, 3), (1, 2), (1, 3), (2, 3), (0, 1), (2, 3))
MIXED = 6
VMEM = pl.BlockSpec(memory_space=pltpu.VMEM)
SMEM = pl.BlockSpec(memory_space=pltpu.SMEM)


def tile_of(pair, second):
    i, j = PAIRS[pair]
    if pair < MIXED:
        return (j, i) if second else (i, j)
    return (j, j) if second else (i, i)


def layout(shape, rows, seq_len):
    n_task, n_z, n_yh, n_x, n_core = shape
    n_y = n_yh * n_task
    flat = np.arange(np.prod(shape)).reshape(shape)
    gather, cube, line = {}, {}, {}
    home = []
    facts = np.zeros((flat.size, 4), np.int32)
    for t, z, yh, x, core in np.ndindex(*shape):
        me = int(flat[t, z, yh, x, core])
        y = yh * n_task + t
        a, m, n = (x, z, y) if core == 0 else ((x + 1) % n_x, (y + 1) % n_y, (z + 1) % n_z)
        pair = m // 2 * 2 + a // 2
        corner = a % 2 * 4 + m % 2 * 2 + n % 2
        step = n // 2
        gather.setdefault((core, a % 2, m % 2, n), {})[pair] = me
        cube.setdefault((core, m // 2, a // 2, n // 2), {})[corner] = me
        line.setdefault((core, a, m, n % 2), {})[step] = me
        i, j = tile_of(pair, corner // 2 % 2)
        to_x = step // 2 * 2 + corner // 4
        to_t = step % 2 * 2 + corner % 2
        home.append((me, int(flat[to_t, 2 * i + j // 2, j % 2, to_x, core])))
        first = (((z * n_yh + yh) * n_x + x) * n_core + core) * rows
        facts[me] = (core, pair < MIXED, first // seq_len, first % seq_len)

    def listed(groups):
        return [[group[k] for k in sorted(group)] for group in groups.values()]

    return listed(gather), listed(cube), listed(line), home, facts


def normed(values, gain, live):
    scale = lax.rsqrt(jnp.mean(values * values, axis=-1, keepdims=True) + 1e-06)
    return (values * scale * gain * live).astype(jnp.bfloat16)


def norm_kernel(facts_ref, lengths_ref, hidden_ref, extra_ref, gain_ref, keep_ref, send_ref):
    rows = hidden_ref.shape[0]
    place = lax.broadcasted_iota(jnp.int32, (rows, 1), 0) + facts_ref[3]
    live = (place < lengths_ref[0, facts_ref[2]]).astype(jnp.float32)
    first = hidden_ref[...].astype(jnp.float32)
    x_attn = normed(first, gain_ref[0:1, :], live)
    mixed = first + extra_ref[...].astype(jnp.float32)
    x_mlp = normed(mixed, gain_ref[1:2, :], live)

    @pl.when(facts_ref[0] == 0)
    def _():
        keep_ref[...] = x_attn
        send_ref[...] = x_mlp

    @pl.when(facts_ref[0] != 0)
    def _():
        keep_ref[...] = x_mlp
        send_ref[...] = x_attn


def norms(facts, lengths, hidden, extra, gains):
    block = jax.ShapeDtypeStruct(hidden.shape, jnp.bfloat16)
    return pl.pallas_call(
        norm_kernel,
        out_shape=(block, block),
        in_specs=[SMEM, SMEM, VMEM, VMEM, VMEM],
        out_specs=(VMEM, VMEM),
    )(facts, lengths, hidden, extra, gains)


def deal_kernel(keep_ref, got_ref, out_ref):
    rows = keep_ref.shape[0]
    band = keep_ref.shape[1] // 4
    for p, pair in enumerate(PAIRS):
        for n, b in enumerate(pair):
            lanes = slice(n * band, (n + 1) * band)
            out_ref[p, :rows, lanes] = keep_ref[:, b * band : (b + 1) * band]
            out_ref[p, rows:, lanes] = got_ref[:, b * band : (b + 1) * band]


def dealt(keep, got):
    rows, width = keep.shape
    return pl.pallas_call(
        deal_kernel,
        out_shape=jax.ShapeDtypeStruct((len(PAIRS), 2 * rows, width // 2), jnp.bfloat16),
        in_specs=[VMEM, VMEM],
        out_specs=VMEM,
    )(keep, got)


def gram_kernel(facts_ref, seen_ref, out_ref):
    band = seen_ref.shape[1] // 2
    rows = band // len(PAIRS)
    for n in range(2):
        at = facts_ref[1] if n == 0 else 1 - facts_ref[1]
        right = seen_ref[:, pl.ds(pl.multiple_of(at * band, 128), band)]
        full = lax.dot_general(
            seen_ref[:, n * band : (n + 1) * band],
            right,
            (((0,), (0,)), ((), ())),
            preferred_element_type=jnp.float32,
        )
        for low_x, low_t in np.ndindex(2, 2):
            pieces = []
            for high_x, high_t, low in np.ndindex(2, 2, 2):
                at = (high_x * 4 + low_x * 2 + low) * rows + (high_t * 2 + low_t) * (rows // 4)
                pieces.append(full[at : at + rows // 4])
            chunk = jnp.concatenate(pieces, axis=0).astype(jnp.bfloat16)
            out_ref[low_x * 4 + n * 2 + low_t] = chunk


def grams(facts, seen):
    band = seen.shape[1] // 2
    return pl.pallas_call(
        gram_kernel,
        out_shape=jax.ShapeDtypeStruct((len(PAIRS), 2 * band // len(PAIRS), band), jnp.bfloat16),
        in_specs=[SMEM, VMEM],
        out_specs=VMEM,
    )(facts, seen)


def solution(mesh):
    shape = (mesh.shape["task"], 8, 2, 4, 2)
    grid = Mesh(mesh.devices.reshape(shape), ALL)

    def per_device(hidden, attn_out, gain_attn, gain_mlp, lengths):
        rows = hidden.shape[1]
        band = hidden.shape[2] // 4
        piece = band // 32
        tokens = rows * lax.axis_size(TOK)
        gather, cube, line, home, table = layout(shape, rows, tokens // lengths.shape[1])
        core = lax.axis_index("core")
        facts = lax.dynamic_index_in_dim(jnp.asarray(table), lax.axis_index(ALL), 0, False)
        gains = jnp.stack([gain_attn, gain_mlp]).astype(jnp.float32)

        def swapped(part, groups):
            return lax.all_to_all(
                part, ALL, split_axis=0, concat_axis=0, axis_index_groups=groups, tiled=True
            )

        def core_swap(part):
            return lax.ppermute(part, "core", [(0, 1), (1, 0)])

        keep, send = norms(facts, lengths, hidden[0], attn_out[0], gains)
        seen = swapped(dealt(keep, core_swap(send)), gather).reshape(-1, 2 * band)
        part = swapped(grams(facts, seen), cube)
        half = part.astype(jnp.float32).sum(axis=0).astype(jnp.bfloat16)
        last = swapped(half.reshape(4, 2 * piece, band), line)
        last = last.astype(jnp.float32).sum(axis=0) * (1.0 / tokens)
        mine = lax.ppermute(last.astype(jnp.bfloat16), ALL, home)
        own = jnp.where(core == 0, mine[:piece], mine[piece:])
        got = core_swap(jnp.where(core == 0, mine[piece:], mine[:piece]))
        out_attn = jnp.where(core == 0, own, got).astype(jnp.float32)
        out_mlp = jnp.where(core == 0, got, own).astype(jnp.float32)
        return out_attn[None], out_mlp[None]

    return jax.shard_map(
        per_device,
        mesh=grid,
        in_specs=(P("task", TOK, None), P("task", TOK, None), P(), P(), P("task", None)),
        out_specs=(P(TOK, "task", None), P(TOK, "task", None)),
        check_vma=False,
    )
```
